128 devices in a mesh: rep: 1, data: 16 (over z, y), expert: 8 (over x, core).
Axes of the slice: x: 4, y: 4, z: 4, core: 2. Of those that a mesh axis runs over, the one named last changes fastest.
Arguments:
- x_tok: bfloat16 [49152, 2048], P(('rep', 'expert', 'data'))
- expert_idx: int32 [49152, 8], P(('rep', 'expert', 'data'))
- gate_val: float32 [49152, 8], P(('rep', 'expert', 'data'))
- w_gate: bfloat16 [128, 2048, 704], P('expert', 'data')
- w_up: bfloat16 [128, 2048, 704], P('expert', 'data')
- w_down: bfloat16 [128, 704, 2048], P('expert', None, 'data')
- ws_gate: bfloat16 [2048, 704], P(('expert', 'data'))
- ws_up: bfloat16 [2048, 704], P(('expert', 'data'))
- ws_down: bfloat16 [704, 2048], P(None, ('expert', 'data'))
Outputs:
- output: bfloat16 [49152, 2048], P(('rep', 'expert', 'data'))
All inputs are finite; a program needn't handle non-finite values.
Results may differ from the reference program's by a relative error of at most 0.00112.
Values are sent between devices in bfloat16 or wider.
A program may use at most 1 GiB of HBM per device.

```python
import jax
import jax.numpy as jnp
from jax import lax

D_MODEL = 2048
FF_EXP = 704
EXPERTS = 128
TOP = 8
FF_SHARED = 704
TOKENS_DEV = 384
BLOCKS = 128
CAPACITY = 32

TOKENS = BLOCKS * TOKENS_DEV
PAIRS = TOKENS_DEV * TOP


def draw_routing(key):
    key_score, key_bias, key_hot = jax.random.split(key, 3)
    scores = jax.random.randint(key_score, (BLOCKS, TOKENS_DEV, EXPERTS), 0, 1024, jnp.int32)
    exp_bias = jax.random.randint(key_bias, (BLOCKS, 1, EXPERTS), 0, 512, jnp.int32)
    hot_expert = jax.random.randint(key_hot, (BLOCKS, 1, 1), 0, EXPERTS, jnp.int32)
    forced = (jnp.arange(TOKENS_DEV, dtype=jnp.int32)[None, :, None] < CAPACITY) & (jnp.arange(EXPERTS, dtype=jnp.int32)[None, None, :] == hot_expert)
    ranked = (scores + exp_bias + jnp.where(forced, 4096, 0)) * EXPERTS + jnp.arange(EXPERTS, dtype=jnp.int32)
    chosen = lax.top_k(ranked, TOP)[1]
    return chosen.reshape(TOKENS, TOP).astype(jnp.int32)


def setup_inputs(seed: int = 0, part: int = 0) -> dict:
    weight_keys = jax.random.split(jax.random.key(seed), 6)
    key_x, key_route, key_gate = jax.random.split(jax.random.fold_in(jax.random.key(seed + 1), part), 3)
    scale_model = D_MODEL ** -0.5
    scale_exp = FF_EXP ** -0.5
    scale_shared = FF_SHARED ** -0.5
    x_tok = jax.random.normal(key_x, (TOKENS, D_MODEL), jnp.float32)
    gate_val = jax.random.uniform(key_gate, (TOKENS, TOP), jnp.float32, 0.2, 0.8)
    w_gate = jax.random.normal(weight_keys[0], (EXPERTS, D_MODEL, FF_EXP), jnp.float32) * scale_model
    w_up = jax.random.normal(weight_keys[1], (EXPERTS, D_MODEL, FF_EXP), jnp.float32) * scale_model
    w_down = jax.random.normal(weight_keys[2], (EXPERTS, FF_EXP, D_MODEL), jnp.float32) * scale_exp
    ws_gate = jax.random.normal(weight_keys[3], (D_MODEL, FF_SHARED), jnp.float32) * scale_model
    ws_up = jax.random.normal(weight_keys[4], (D_MODEL, FF_SHARED), jnp.float32) * scale_model
    ws_down = jax.random.normal(weight_keys[5], (FF_SHARED, D_MODEL), jnp.float32) * scale_shared
    return {"x_tok": x_tok.astype(jnp.bfloat16), "expert_idx": draw_routing(key_route), "gate_val": gate_val, "w_gate": w_gate.astype(jnp.bfloat16), "w_up": w_up.astype(jnp.bfloat16), "w_down": w_down.astype(jnp.bfloat16), "ws_gate": ws_gate.astype(jnp.bfloat16), "ws_up": ws_up.astype(jnp.bfloat16), "ws_down": ws_down.astype(jnp.bfloat16)}


def slot_block(flat_idx):
    onehot = (flat_idx[:, None] == jnp.arange(EXPERTS, dtype=jnp.int32)[None, :]).astype(jnp.int32)
    slot_idx = jnp.sum((jnp.cumsum(onehot, axis=0) - onehot) * onehot, axis=1)
    return jnp.where(slot_idx < CAPACITY, flat_idx * CAPACITY + slot_idx, EXPERTS * CAPACITY)


def source_block(dest_pos):
    return jnp.full((EXPERTS * CAPACITY,), PAIRS, jnp.int32).at[dest_pos].set(jnp.arange(PAIRS, dtype=jnp.int32), mode="drop")


def expert_ffn(tok_rows, w_gate, w_up, w_down):
    gate_pre = jnp.dot(tok_rows, w_gate, preferred_element_type=jnp.float32)
    up_pre = jnp.dot(tok_rows, w_up, preferred_element_type=jnp.float32)
    hidden = (jax.nn.silu(gate_pre) * up_pre).astype(jnp.bfloat16)
    return jnp.dot(hidden, w_down, preferred_element_type=jnp.float32).astype(jnp.bfloat16)


def reference(x_tok, expert_idx, gate_val, w_gate, w_up, w_down, ws_gate, ws_up, ws_down):
    dest_pos = jax.vmap(slot_block)(expert_idx.reshape(BLOCKS, PAIRS))
    src_pair = jax.vmap(source_block)(dest_pos)
    filled = src_pair < PAIRS
    glob_pair = jnp.minimum(src_pair, PAIRS - 1) + PAIRS * jnp.arange(BLOCKS, dtype=jnp.int32)[:, None]
    slot_gate = jnp.where(filled, gate_val.reshape(BLOCKS * PAIRS)[glob_pair], 0.0)

    def by_expert(id_table):
        return id_table.reshape(BLOCKS, EXPERTS, CAPACITY).transpose(1, 0, 2).reshape(EXPERTS, BLOCKS * CAPACITY)

    def expert_step(routed, per_expert):
        wg_e, wu_e, wd_e, tok_ids, fill_e, gate_e = per_expert
        tok_rows = jnp.where(fill_e[:, None], x_tok[tok_ids], jnp.zeros((), x_tok.dtype))
        out_rows = expert_ffn(tok_rows, wg_e, wu_e, wd_e)
        return routed.at[tok_ids].add(gate_e[:, None] * out_rows.astype(jnp.float32)), None

    routed = lax.scan(expert_step, jnp.zeros((TOKENS, D_MODEL), jnp.float32), (w_gate, w_up, w_down, by_expert(glob_pair // TOP), by_expert(filled), by_expert(slot_gate)))[0]

    def shared_of(x_blk):
        gate_pre = jnp.dot(x_blk, ws_gate, preferred_element_type=jnp.float32)
        up_pre = jnp.dot(x_blk, ws_up, preferred_element_type=jnp.float32)
        hidden = (jax.nn.silu(gate_pre) * up_pre).astype(jnp.bfloat16)
        return jnp.dot(hidden, ws_down, preferred_element_type=jnp.float32)

    shared = lax.map(shared_of, x_tok.reshape(BLOCKS, TOKENS_DEV, D_MODEL)).reshape(TOKENS, D_MODEL)
    return (x_tok.astype(jnp.float32) + shared + routed).astype(jnp.bfloat16)
```

```python
import jax
import jax.numpy as jnp
from jax import lax
from jax.sharding import PartitionSpec as P

CAP_NUM = 5
CAP_DEN = 4


def capacity_of(tok_count, top_count, n_exp):
    return max(8, ((CAP_NUM * top_count * tok_count) // (CAP_DEN * n_exp) + 7) // 8 * 8)


def routing(idx_loc, gate_loc, n_exp, capacity):
    tok_count = idx_loc.shape[0]
    hit = idx_loc[:, :, None] == jnp.arange(n_exp, dtype=jnp.int32)[None, None, :]
    chosen = jnp.any(hit, axis=1)
    gates = jnp.sum(jnp.where(hit, gate_loc[:, :, None], 0.0), axis=1)
    before = jnp.tril(jnp.ones((tok_count, tok_count), jnp.bfloat16), -1)
    slot = jnp.dot(before, chosen.astype(jnp.bfloat16), preferred_element_type=jnp.float32).astype(jnp.int32)
    slot = jnp.where(chosen & (slot < capacity), slot, capacity)
    return slot.T, gates.T


def split3(val):
    hi = lax.reduce_precision(val, 8, 7)
    mid = lax.reduce_precision(val - hi, 8, 7)
    low = val - hi - mid
    return [part.astype(jnp.bfloat16) for part in (hi, mid, low)]


def solution(mesh):
    exp_n = mesh.shape["expert"]
    data_n = mesh.shape["data"]
    tok_spec = P(("rep", "expert", "data"), None)
    group_axes = ("expert", "data")

    def device_fn(x_loc, idx_loc, gate_loc, wg_loc, wu_loc, wd_loc, wsg_loc, wsu_loc, wsd_loc):
        tok_count, d_model = x_loc.shape
        n_exp = wg_loc.shape[0] * exp_n
        ff = wg_loc.shape[2]
        capacity = capacity_of(tok_count, idx_loc.shape[1], n_exp)
        w_gate = lax.all_to_all(wg_loc, "data", 0, 1, tiled=True).reshape(d_model, ff)
        w_up = lax.all_to_all(wu_loc, "data", 0, 1, tiled=True).reshape(d_model, ff)
        w_down = lax.all_to_all(wd_loc, "data", 0, 0, tiled=True)
        w_down = w_down.reshape(data_n, ff, d_model // data_n)
        slot, gates = routing(idx_loc, gate_loc, n_exp, capacity)
        sel = slot[:, None, :] == jnp.arange(capacity, dtype=jnp.int32)[None, :, None]
        pick = sel.astype(jnp.bfloat16).reshape(n_exp * capacity, tok_count)
        buffer = jnp.dot(pick, x_loc, preferred_element_type=jnp.float32).astype(jnp.bfloat16)
        received = lax.all_to_all(buffer.reshape(n_exp, capacity, d_model), group_axes, 0, 0, tiled=True)
        rows = received.reshape(n_exp * capacity, d_model)
        gate_pre = jnp.dot(rows, w_gate, preferred_element_type=jnp.float32)
        up_pre = jnp.dot(rows, w_up, preferred_element_type=jnp.float32)
        hidden = (jax.nn.silu(gate_pre) * up_pre).astype(jnp.bfloat16)
        w_down = jnp.transpose(w_down, (1, 0, 2)).reshape(ff, d_model)
        expert_out = jnp.dot(hidden, w_down, preferred_element_type=jnp.float32).astype(jnp.bfloat16)
        returned = lax.all_to_all(expert_out.reshape(n_exp, capacity, d_model), group_axes, 0, 0, tiled=True)
        returned = returned.reshape(n_exp * capacity, d_model)
        ws_gate = lax.all_gather(wsg_loc, group_axes, axis=0, tiled=True)
        ws_up = lax.all_gather(wsu_loc, group_axes, axis=0, tiled=True)
        ws_down = lax.all_gather(wsd_loc, group_axes, axis=1, tiled=True)
        s_gate = jnp.dot(x_loc, ws_gate, preferred_element_type=jnp.float32)
        s_up = jnp.dot(x_loc, ws_up, preferred_element_type=jnp.float32)
        s_hidden = (jax.nn.silu(s_gate) * s_up).astype(jnp.bfloat16)
        total = jnp.dot(s_hidden, ws_down, preferred_element_type=jnp.float32) + x_loc.astype(jnp.float32)
        for part in split3(gates):
            weight = jnp.where(sel, part[:, None, :], jnp.zeros((), jnp.bfloat16)).reshape(n_exp * capacity, tok_count)
            total += lax.dot_general(weight, returned, (((0,), (0,)), ((), ())), preferred_element_type=jnp.float32)
        return total.astype(jnp.bfloat16)

    in_specs = (tok_spec, tok_spec, tok_spec, P("expert", "data", None), P("expert", "data", None), P("expert", None, "data"), P(group_axes, None), P(group_axes, None), P(None, group_axes))
    return jax.shard_map(device_fn, mesh=mesh, in_specs=in_specs, out_specs=tok_spec, check_vma=False)
```

```python
import jax
import jax.numpy as jnp
from jax import lax
from jax.experimental import pallas as pl
from jax.experimental.pallas import tpu as pltpu
from jax.sharding import PartitionSpec as P

MESH = pl.DeviceIdType.MESH
CAP_NUM = 5
CAP_DEN = 4
SIDE = 4


def capacity_of(tok_count, top_count, n_exp):
    return max(8, ((CAP_NUM * top_count * tok_count) // (CAP_DEN * n_exp) + 7) // 8 * 8)


def routing(idx_loc, gate_loc, n_exp, capacity):
    tok_count = idx_loc.shape[0]
    hit = idx_loc[:, :, None] == jnp.arange(n_exp, dtype=jnp.int32)[None, None, :]
    chosen = jnp.any(hit, axis=1)
    gates = jnp.sum(jnp.where(hit, gate_loc[:, :, None], 0.0), axis=1)
    before = jnp.tril(jnp.ones((tok_count, tok_count), jnp.bfloat16), -1)
    slot = jnp.dot(before, chosen.astype(jnp.bfloat16), preferred_element_type=jnp.float32).astype(jnp.int32)
    slot = jnp.where(chosen & (slot < capacity), slot, capacity)
    return slot.T, gates.T


def split3(val):
    hi = lax.reduce_precision(val, 8, 7)
    mid = lax.reduce_precision(val - hi, 8, 7)
    low = val - hi - mid
    return [part.astype(jnp.bfloat16) for part in (hi, mid, low)]


def moe_kernel(buf, wg, wu, wd, ret, xr, wgu_v, wd_v, x_v, o_v,
               w1s, w1r, w2s, w2r, w3s, w3r, lws, ds, dr, rs, rls, rr, xs, own):
    n_own = SIDE
    blk = wg.shape[1]
    n_src = xr.shape[1]
    half = x_v.shape[1]
    cap, d_model = buf.shape[1], buf.shape[2]
    d = lax.axis_index("data")
    p = lax.axis_index("expert")
    z, y = lax.div(d, SIDE), lax.rem(d, SIDE)
    x, c = lax.div(p, 2), lax.rem(p, 2)
    u = z * (1 - c) + y * c
    v = y * (1 - c) + z * c

    def data_of(uu, vv):
        return uu * (SIDE - 3 * c) + vv * (1 + 3 * c)

    v_up, v_dn = lax.rem(v + 1, SIDE), lax.rem(v + SIDE - 1, SIDE)

    def send(src, dst, s_sem, r_sem, data, expert):
        pltpu.make_async_remote_copy(src, dst, s_sem, r_sem, device_id={"data": data, "expert": expert}, device_id_type=MESH).start()

    def wait(ref, sem):
        pltpu.make_async_copy(ref, ref, sem).wait()

    def gu_block(e, b):
        return wgu_v.at[e, :, pl.ds(pl.multiple_of(b * blk, blk), blk), :]

    def gu_part(e, i, b):
        return wgu_v.at[e, i, pl.ds(pl.multiple_of(b * blk, blk), blk), :]

    def d_block(e, b):
        return wd_v.at[e, :, pl.ds(pl.multiple_of(b * blk, blk), blk)]

    def start_trade(e):
        own_e = n_own * u + e
        pltpu.make_async_copy(wg.at[own_e], gu_part(e, 0, d), lws.at[e, 0]).start()
        pltpu.make_async_copy(wu.at[own_e], gu_part(e, 1, d), lws.at[e, 1]).start()
        pltpu.make_async_copy(wd.at[own_e], d_block(e, d), lws.at[e, 2]).start()
        for r in range(1, SIDE):
            ut = lax.rem(u + r, SIDE)
            te = n_own * ut + e
            td = data_of(ut, v)
            send(wg.at[te], gu_part(e, 0, d), w1s.at[e, 0], w1r.at[e, 0], td, p)
            send(wu.at[te], gu_part(e, 1, d), w1s.at[e, 0], w1r.at[e, 0], td, p)
            send(wd.at[te], d_block(e, d), w1s.at[e, 1], w1r.at[e, 1], td, p)

    def start_rows(e):
        def body(k, carry):
            dx, cb, r = lax.div(k, 8), lax.rem(lax.div(k, SIDE), 2), lax.rem(k, SIDE)
            tx, tc = lax.rem(x + dx, SIDE), lax.rem(c + cb, 2)
            tz = lax.rem(z + r * (1 - tc), SIDE)
            ty = lax.rem(y + r * tc, SIDE)
            tp = tx * 2 + tc
            te = tp * (SIDE * n_own) + n_own * (tz * (1 - tc) + ty * tc) + e
            send(buf.at[te], xr.at[e, k], ds.at[e], dr.at[e], tz * SIDE + ty, tp)
            return carry

        lax.fori_loop(1, n_src, body, 0)

    def start_gather(e):
        pltpu.make_async_copy(wg.at[0], gu_part(e, 0, d), lws.at[e, 0]).wait()
        pltpu.make_async_copy(wu.at[0], gu_part(e, 1, d), lws.at[e, 1]).wait()
        pltpu.make_async_copy(wd.at[0], d_block(e, d), lws.at[e, 2]).wait()
        wait(wgu_v.at[e, :, pl.ds(0, 3 * blk), :], w1r.at[e, 0])
        wait(wd_v.at[e, :, pl.ds(0, 3 * blk)], w1r.at[e, 1])
        for i in range(SIDE):
            b = data_of(i, v)
            for vt in (v_up, v_dn):
                send(gu_block(e, b), gu_block(e, b), w2s.at[e, 0], w2r.at[e, 0], data_of(u, vt), p)
                send(d_block(e, b), d_block(e, b), w2s.at[e, 1], w2r.at[e, 1], data_of(u, vt), p)

    def start_relay(e):
        wait(wgu_v.at[e, :, pl.ds(0, 8 * blk), :], w2r.at[e, 0])
        wait(wd_v.at[e, :, pl.ds(0, 8 * blk)], w2r.at[e, 1])
        for i in range(SIDE):
            vs, vt = (v_dn, v_up) if i < SIDE // 2 else (v_up, v_dn)
            b = data_of(i, vs)
            send(gu_block(e, b), gu_block(e, b), w3s.at[e, 0], w3r.at[e, 0], data_of(u, vt), p)
            send(d_block(e, b), d_block(e, b), w3s.at[e, 1], w3r.at[e, 1], data_of(u, vt), p)

    def load(e, sb):
        return pltpu.make_async_copy(xr.at[e, pl.ds(sb * half, half)], x_v.at[sb], xs.at[sb])

    def experts(e, slot):
        wait(wgu_v.at[e, :, pl.ds(0, 4 * blk), :], w3r.at[e, 0])
        wait(wd_v.at[e, :, pl.ds(0, 4 * blk)], w3r.at[e, 1])
        wait(xr.at[e, pl.ds(1, n_src - 1)], dr.at[e])
        parts = n_src // half
        for sb in range(parts):
            load(e, sb).start()
        for sb in range(parts):
            load(e, sb).wait()
            rows = x_v[sb].reshape(half * cap, d_model)
            gate_pre = jnp.dot(rows, wgu_v[e, 0], preferred_element_type=jnp.float32)
            up_pre = jnp.dot(rows, wgu_v[e, 1], preferred_element_type=jnp.float32)
            hidden = (jax.nn.silu(gate_pre) * up_pre).astype(jnp.bfloat16)
            res = jnp.dot(hidden, wd_v[e], preferred_element_type=jnp.float32).astype(jnp.bfloat16)
            o_v[slot, pl.ds(sb * half, half)] = res.reshape(half, cap, d_model)
        my_e = p * (SIDE * n_own) + n_own * u + e

        def body(k, carry):
            dx, cb, r = lax.div(k, 8), lax.rem(lax.div(k, SIDE), 2), lax.rem(k, SIDE)
            sp = lax.rem(x + SIDE - dx, SIDE) * 2 + lax.rem(c + cb, 2)
            sd = data_of(lax.rem(u + SIDE - r, SIDE), v)
            send(o_v.at[slot, k], ret.at[my_e], rs.at[slot], rr, sd, sp)
            return carry

        lax.fori_loop(1, n_src, body, 0)
        pltpu.make_async_copy(o_v.at[slot, 0], ret.at[my_e], rls.at[slot]).start()

    def wait_results(slot):
        wait(o_v.at[slot, pl.ds(1, n_src - 1)], rs.at[slot])
        pltpu.make_async_copy(o_v.at[slot, 0], ret.at[0], rls.at[slot]).wait()

    def own_rows():
        return pltpu.make_async_copy(buf.at[pl.ds(p * (SIDE * n_own) + n_own * u, n_own)], xr.at[:, 0], own)

    own_rows().start()
    start_trade(0)
    start_rows(0)
    start_trade(1)
    start_rows(1)
    start_gather(0)
    start_trade(2)
    start_rows(2)
    start_relay(0)
    start_gather(1)
    start_trade(3)
    start_rows(3)
    own_rows().wait()

    def step(e, carry):
        slot = lax.rem(e, 2)

        @pl.when(e >= 2)
        def _():
            wait_results(slot)

        experts(e, slot)

        @pl.when(e + 1 < n_own)
        def _():
            start_relay(e + 1)

        @pl.when(e + 2 < n_own)
        def _():
            start_gather(e + 2)

        return carry

    lax.fori_loop(0, n_own, step, 0)
    for slot in range(2):
        wait_results(slot)
    wait(ret.at[pl.ds(0, n_own * (n_src - 1))], rr)

    def drain(e, carry):
        wait(wgu_v.at[e, :, pl.ds(0, 3 * blk), :], w1s.at[e, 0])
        wait(wd_v.at[e, :, pl.ds(0, 3 * blk)], w1s.at[e, 1])
        wait(wgu_v.at[e, :, pl.ds(0, 8 * blk), :], w2s.at[e, 0])
        wait(wd_v.at[e, :, pl.ds(0, 8 * blk)], w2s.at[e, 1])
        wait(wgu_v.at[e, :, pl.ds(0, 4 * blk), :], w3s.at[e, 0])
        wait(wd_v.at[e, :, pl.ds(0, 4 * blk)], w3s.at[e, 1])
        wait(xr.at[e, pl.ds(1, n_src - 1)], ds.at[e])
        return carry

    lax.fori_loop(0, n_own, drain, 0)


def moe(buffer, wg_loc, wu_loc, wd_loc):
    n_exp, cap, d_model = buffer.shape
    n_loc, blk, ff = wg_loc.shape
    n_own, n_src = SIDE, 8 * SIDE
    dma = pltpu.SemaphoreType.DMA
    bf16 = jnp.bfloat16
    any_spec = pl.BlockSpec(memory_space=pl.ANY)
    return pl.pallas_call(
        moe_kernel,
        out_shape=(jax.ShapeDtypeStruct(buffer.shape, bf16), jax.ShapeDtypeStruct((n_own, n_src, cap, d_model), bf16)),
        in_specs=[any_spec] * 4,
        out_specs=(any_spec, any_spec),
        scratch_shapes=[
            pltpu.VMEM((n_own, 2, d_model, ff), bf16),
            pltpu.VMEM((n_own, ff, d_model), bf16),
            pltpu.VMEM((2, n_src // 2, cap, d_model), bf16),
            pltpu.VMEM((2, n_src, cap, d_model), bf16),
        ] + [dma((n_own, 2))] * 6 + [dma((n_own, 3)), dma((n_own,)), dma((n_own,)), dma((2,)), dma((2,)), dma, dma((2,)), dma],
        compiler_params=pltpu.CompilerParams(has_side_effects=True, vmem_limit_bytes=64000 * 1024),
        cost_estimate=pl.CostEstimate(flops=6 * n_exp * cap * d_model * ff * 10, bytes_accessed=100_000_000, transcendentals=n_exp * cap * ff),
        name="moe_exchange",
    )(buffer, wg_loc, wu_loc, wd_loc)[0]


def solution(mesh):
    exp_n = mesh.shape["expert"]
    tok_spec = P(("rep", "expert", "data"), None)
    group_axes = ("expert", "data")

    def device_fn(x_loc, idx_loc, gate_loc, wg_loc, wu_loc, wd_loc, wsg_loc, wsu_loc, wsd_loc):
        tok_count, d_model = x_loc.shape
        n_exp = wg_loc.shape[0] * exp_n
        ff_shared = wsg_loc.shape[1]
        capacity = capacity_of(tok_count, idx_loc.shape[1], n_exp)
        ws_loc = jnp.concatenate([wsg_loc, wsu_loc, wsd_loc.T], axis=1)
        ws_all = lax.all_gather(ws_loc, group_axes, axis=0, tiled=True)
        slot, gates = routing(idx_loc, gate_loc, n_exp, capacity)
        sel = slot[:, None, :] == jnp.arange(capacity, dtype=jnp.int32)[None, :, None]
        pick = sel.astype(jnp.bfloat16).reshape(n_exp * capacity, tok_count)
        buffer = jnp.dot(pick, x_loc, preferred_element_type=jnp.float32).astype(jnp.bfloat16)
        returned = moe(buffer.reshape(n_exp, capacity, d_model), wg_loc, wu_loc, wd_loc)
        returned = returned.reshape(n_exp * capacity, d_model)
        s_gate = jnp.dot(x_loc, ws_all[:, :ff_shared], preferred_element_type=jnp.float32)
        s_up = jnp.dot(x_loc, ws_all[:, ff_shared:2 * ff_shared], preferred_element_type=jnp.float32)
        s_hidden = (jax.nn.silu(s_gate) * s_up).astype(jnp.bfloat16)
        total = lax.dot_general(s_hidden, ws_all[:, 2 * ff_shared:], (((1,), (1,)), ((), ())), preferred_element_type=jnp.float32)
        total += x_loc.astype(jnp.float32)
        for part in split3(gates):
            weight = jnp.where(sel, part[:, None, :], jnp.zeros((), jnp.bfloat16)).reshape(n_exp * capacity, tok_count)
            total += lax.dot_general(weight, returned, (((0,), (0,)), ((), ())), preferred_element_type=jnp.float32)
        return total.astype(jnp.bfloat16)

    in_specs = (tok_spec, tok_spec, tok_spec, P("expert", "data", None), P("expert", "data", None), P("expert", None, "data"), P(group_axes, None), P(group_axes, None), P(None, group_axes))
    return jax.shard_map(device_fn, mesh=mesh, in_specs=in_specs, out_specs=tok_spec, check_vma=False)
```

```python
import jax
import jax.numpy as jnp
from jax import lax
from jax.experimental import pallas as pl
from jax.experimental.pallas import tpu as pltpu
from jax.sharding import PartitionSpec as P

MESH = pl.DeviceIdType.MESH
CAP_NUM = 5
CAP_DEN = 4
SIDE = 4


def capacity_of(tok_count, top_count, n_exp):
    return max(8, ((CAP_NUM * top_count * tok_count) // (CAP_DEN * n_exp) + 7) // 8 * 8)


def routing(idx_loc, gate_loc, n_exp, capacity):
    tok_count = idx_loc.shape[0]
    hit = idx_loc[:, :, None] == jnp.arange(n_exp, dtype=jnp.int32)[None, None, :]
    chosen = jnp.any(hit, axis=1)
    gates = jnp.sum(jnp.where(hit, gate_loc[:, :, None], 0.0), axis=1)
    before = jnp.tril(jnp.ones((tok_count, tok_count), jnp.bfloat16), -1)
    slot = jnp.dot(before, chosen.astype(jnp.bfloat16), preferred_element_type=jnp.float32).astype(jnp.int32)
    slot = jnp.where(chosen & (slot < capacity), slot, capacity)
    return slot.T, gates.T


def moe_kernel(x_in, slot_in, gate_in, wg, wu, wd, acc, xr, ret, w_v, pool, x_v, t_v,
               w1s, w1r, w2s, w2r, w3s, w3r, lws, ds, dr, rs, rls, rr, xs, own):
    n_own = SIDE
    blk = wg.shape[2]
    n_src, cap, d_model = xr.shape[1:]
    tok_count = x_in.shape[0]
    unit = x_v.shape[1]
    units = n_src // unit
    d = lax.axis_index("data")
    p = lax.axis_index("expert")
    z, y = lax.div(d, SIDE), lax.rem(d, SIDE)
    x, c = lax.div(p, 2), lax.rem(p, 2)
    u = z * (1 - c) + y * c
    v = y * (1 - c) + z * c
    v_up, v_dn = lax.rem(v + 1, SIDE), lax.rem(v + SIDE - 1, SIDE)
    slots = lax.broadcasted_iota(jnp.int32, (cap, tok_count), 0)

    def data_of(uu, vv):
        return uu * (SIDE - 3 * c) + vv * (1 + 3 * c)

    def target(k):
        dx, cb, r = lax.div(k, 8), lax.rem(lax.div(k, SIDE), 2), lax.rem(k, SIDE)
        tx, tc = lax.rem(x + dx, SIDE), lax.rem(c + cb, 2)
        tz = lax.rem(z + r * (1 - tc), SIDE)
        ty = lax.rem(y + r * tc, SIDE)
        tp = tx * 2 + tc
        return tp, tz * SIDE + ty, tp * (SIDE * n_own) + n_own * (tz * (1 - tc) + ty * tc)

    def source(k):
        dx, cb, r = lax.div(k, 8), lax.rem(lax.div(k, SIDE), 2), lax.rem(k, SIDE)
        sp = lax.rem(x + SIDE - dx, SIDE) * 2 + lax.rem(c + cb, 2)
        return sp, data_of(lax.rem(u + SIDE - r, SIDE), v)

    def send(src, dst, s_sem, r_sem, data, expert):
        pltpu.make_async_remote_copy(src, dst, s_sem, r_sem, device_id={"data": data, "expert": expert}, device_id_type=MESH).start()

    def wait(ref, sem):
        pltpu.make_async_copy(ref, ref, sem).wait()

    def strips(e, count):
        return w_v.at[e, :, :, pl.ds(0, count * blk)]

    def strip(e, b):
        return w_v.at[e, :, :, pl.ds(pl.multiple_of(b * blk, blk), blk)]

    def part(e, i, b):
        return w_v.at[e, i, :, pl.ds(pl.multiple_of(b * blk, blk), blk)]

    def start_trade(e):
        for i, w in enumerate((wg, wu, wd)):
            pltpu.make_async_copy(w.at[n_own * u + e], part(e, i, d), lws.at[e, i]).start()
        for r in range(1, SIDE):
            ut = lax.rem(u + r, SIDE)
            for i, w in enumerate((wg, wu, wd)):
                send(w.at[n_own * ut + e], part(e, i, d), w1s.at[e], w1r.at[e], data_of(ut, v), p)

    def start_rows(e, slot):
        def pick(g, carry):
            for j in range(unit):
                te = target(g * unit + j)[2] + e
                t_v[0, j * cap:(j + 1) * cap, :] = (slots == slot_in[pl.ds(te, 1), :]).astype(jnp.bfloat16)
            rows = jnp.dot(t_v[0], x_in[...], preferred_element_type=jnp.float32).astype(jnp.bfloat16)
            pool[slot, pl.ds(g * unit, unit)] = rows.reshape(unit, cap, d_model)
            return carry

        lax.fori_loop(0, units, pick, 0)

        def body(k, carry):
            tp, td, _ = target(k)
            send(pool.at[slot, k], xr.at[e, k], ds.at[e], dr.at[e], td, tp)
            return carry

        lax.fori_loop(1, n_src, body, 0)
        pltpu.make_async_copy(pool.at[slot, 0], xr.at[e, 0], own.at[e]).start()

    def wait_rows_sent(e, slot):
        wait(pool.at[slot, pl.ds(1, n_src - 1)], ds.at[e])
        pltpu.make_async_copy(pool.at[slot, 0], xr.at[e, 0], own.at[e]).wait()

    def start_gather(e):
        for i, w in enumerate((wg, wu, wd)):
            pltpu.make_async_copy(w.at[0], part(e, i, d), lws.at[e, i]).wait()
        wait(strips(e, 3), w1r.at[e])
        for i in range(SIDE):
            b = data_of(i, v)
            for vt in (v_up, v_dn):
                send(strip(e, b), strip(e, b), w2s.at[e], w2r.at[e], data_of(u, vt), p)

    def start_relay(e):
        wait(strips(e, 8), w2r.at[e])
        for i in range(SIDE):
            vs, vt = (v_dn, v_up) if i < SIDE // 2 else (v_up, v_dn)
            b = data_of(i, vs)
            send(strip(e, b), strip(e, b), w3s.at[e], w3r.at[e], data_of(u, vt), p)

    def load(src, e, g, s):
        return pltpu.make_async_copy(src.at[e, pl.ds(g * unit, unit)], x_v.at[s], xs.at[s])

    def streamed(src, e, work):
        load(src, e, 0, 0).start()

        def body(g, carry):
            s = lax.rem(g, 2)

            @pl.when(g + 1 < units)
            def _():
                load(src, e, g + 1, 1 - s).start()

            load(src, e, g, s).wait()
            work(g, x_v[s].reshape(unit * cap, d_model))
            return carry

        lax.fori_loop(0, units, body, 0)

    def give_back(e, slot, k):
        sp, sd = source(k)
        send(pool.at[slot, k], ret.at[e, k], rs.at[e], rr.at[e], sd, sp)

    def experts(e, slot):
        wait(strips(e, 4), w3r.at[e])
        wait(xr.at[e, pl.ds(1, n_src - 1)], dr.at[e])
        nt = (((1,), (1,)), ((), ()))

        def send_unit(g):
            for j in range(unit):
                give_back(e, slot, g * unit + j)

        def work(g, rows):
            gate_pre = lax.dot_general(rows, w_v[e, 0], nt, preferred_element_type=jnp.float32)
            up_pre = lax.dot_general(rows, w_v[e, 1], nt, preferred_element_type=jnp.float32)
            hidden = (jax.nn.silu(gate_pre) * up_pre).astype(jnp.bfloat16)
            res = jnp.dot(hidden, w_v[e, 2], preferred_element_type=jnp.float32).astype(jnp.bfloat16)
            pool[slot, pl.ds(g * unit, unit)] = res.reshape(unit, cap, d_model)

            @pl.when(g == 1)
            def _():
                for j in range(1, unit):
                    give_back(e, slot, j)

            @pl.when(g > 1)
            def _():
                send_unit(g - 1)

        streamed(xr, e, work)
        send_unit(units - 1)
        pltpu.make_async_copy(pool.at[slot, 0], ret.at[e, 0], rls.at[e]).start()

    def wait_results_sent(e, slot):
        wait(pool.at[slot, pl.ds(1, n_src - 1)], rs.at[e])

    def combine(e):
        wait(ret.at[e, pl.ds(1, n_src - 1)], rr.at[e])
        pltpu.make_async_copy(pool.at[0, 0], ret.at[e, 0], rls.at[e]).wait()
        tn = (((0,), (0,)), ((), ()))
        width = d_model // 4

        def work(g, rows):
            for j in range(unit):
                te = target(g * unit + j)[2] + e
                val = jnp.where(slots == slot_in[pl.ds(te, 1), :], gate_in[pl.ds(te, 1), :], 0.0)
                hi = val.astype(jnp.bfloat16)
                rest = val - hi.astype(jnp.float32)
                mid = rest.astype(jnp.bfloat16)
                low = (rest - mid.astype(jnp.float32)).astype(jnp.bfloat16)
                for i, term in enumerate((hi, mid, low)):
                    t_v[i, j * cap:(j + 1) * cap, :] = term
            for n in range(4):
                cols = rows[:, n * width:(n + 1) * width]
                total = acc[:, n * width:(n + 1) * width]
                for i in range(3):
                    total += lax.dot_general(t_v[i], cols, tn, preferred_element_type=jnp.float32)
                acc[:, n * width:(n + 1) * width] = total

        streamed(ret, e, work)

    start_trade(0)
    start_rows(0, 0)
    start_trade(1)
    start_rows(1, 1)
    acc[...] = jnp.zeros_like(acc)
    start_gather(0)
    start_trade(2)
    start_rows(2, 2)
    start_relay(0)
    start_gather(1)
    start_trade(3)
    wait_rows_sent(0, 0)
    start_rows(3, 0)

    def step(e, carry):
        slot = lax.rem(e + 1, 3)

        @pl.when(e < 3)
        def _():
            wait_rows_sent(e + 1, slot)

        @pl.when(e == 3)
        def _():
            wait_results_sent(0, 1)

        experts(e, slot)

        @pl.when(e + 1 < n_own)
        def _():
            start_relay(e + 1)

        @pl.when(e + 2 < n_own)
        def _():
            start_gather(e + 2)

        @pl.when(e >= 1)
        def _():
            combine(e - 1)

        return carry

    lax.fori_loop(0, n_own, step, 0)
    for e in range(1, n_own):
        wait_results_sent(e, (e + 1) % 3)
    combine(n_own - 1)

    def drain(e, carry):
        wait(strips(e, 3), w1s.at[e])
        wait(strips(e, 8), w2s.at[e])
        wait(strips(e, 4), w3s.at[e])
        return carry

    lax.fori_loop(0, n_own, drain, 0)


def moe(x_loc, slot, gates, wg_loc, wu_loc, wd_loc, cap):
    tok_count, d_model = x_loc.shape
    n_loc, blk, ff = wg_loc.shape
    n_exp = slot.shape[0]
    n_own, n_src, unit = SIDE, 8 * SIDE, 8
    dma = pltpu.SemaphoreType.DMA
    bf16 = jnp.bfloat16
    any_spec = pl.BlockSpec(memory_space=pl.ANY)
    vmem_spec = pl.BlockSpec(memory_space=pltpu.VMEM)
    stage = jax.ShapeDtypeStruct((n_own, n_src, cap, d_model), bf16)
    return pl.pallas_call(
        moe_kernel,
        out_shape=(jax.ShapeDtypeStruct((tok_count, d_model), jnp.float32), stage, stage),
        in_specs=[vmem_spec] * 3 + [any_spec] * 3,
        out_specs=(vmem_spec, any_spec, any_spec),
        scratch_shapes=[
            pltpu.VMEM((n_own, 3, ff, d_model), bf16),
            pltpu.VMEM((3, n_src, cap, d_model), bf16),
            pltpu.VMEM((2, unit, cap, d_model), bf16),
            pltpu.VMEM((3, unit * cap, tok_count), bf16),
        ] + [dma((n_own,))] * 6 + [dma((n_own, 3))] + [dma((n_own,))] * 5 + [dma((2,)), dma((n_own,))],
        compiler_params=pltpu.CompilerParams(has_side_effects=True, vmem_limit_bytes=65400 * 1024),
        cost_estimate=pl.CostEstimate(flops=60 * n_exp * cap * d_model * ff, bytes_accessed=100_000_000, transcendentals=n_exp * cap * ff),
        name="moe_exchange",
    )(x_loc, slot, gates, jnp.swapaxes(wg_loc, 1, 2), jnp.swapaxes(wu_loc, 1, 2), wd_loc)[0]


def solution(mesh):
    exp_n = mesh.shape["expert"]
    tok_spec = P(("rep", "expert", "data"), None)
    group_axes = ("expert", "data")

    def device_fn(x_loc, idx_loc, gate_loc, wg_loc, wu_loc, wd_loc, wsg_loc, wsu_loc, wsd_loc):
        tok_count, d_model = x_loc.shape
        n_exp = wg_loc.shape[0] * exp_n
        ff_shared = wsg_loc.shape[1]
        capacity = capacity_of(tok_count, idx_loc.shape[1], n_exp)
        ws_loc = jnp.concatenate([wsg_loc, wsu_loc, wsd_loc.T], axis=1)
        ws_all = lax.all_gather(ws_loc, group_axes, axis=0, tiled=True)
        slot, gates = routing(idx_loc, gate_loc, n_exp, capacity)
        routed = moe(x_loc, slot, gates, wg_loc, wu_loc, wd_loc, capacity)
        pre = jnp.dot(x_loc, ws_all[:, :2 * ff_shared], preferred_element_type=jnp.float32)
        s_hidden = (jax.nn.silu(pre[:, :ff_shared]) * pre[:, ff_shared:]).astype(jnp.bfloat16)
        shared = lax.dot_general(s_hidden, ws_all[:, 2 * ff_shared:], (((1,), (1,)), ((), ())), preferred_element_type=jnp.float32)
        return (x_loc.astype(jnp.float32) + shared + routed).astype(jnp.bfloat16)

    in_specs = (tok_spec, tok_spec, tok_spec, P("expert", "data", None), P("expert", "data", None), P("expert", None, "data"), P(group_axes, None), P(group_axes, None), P(None, group_axes))
    return jax.shard_map(device_fn, mesh=mesh, in_specs=in_specs, out_specs=tok_spec, check_vma=False)
```

```python
import jax
import jax.numpy as jnp
from jax import lax
from jax.experimental import pallas as pl
from jax.experimental.pallas import tpu as pltpu
from jax.sharding import PartitionSpec as P

MESH = pl.DeviceIdType.MESH
OWN = 24
CAP_NUM = 5
CAP_DEN = 4
SIDE = 4


def capacity_of(tok_count, top_count, n_exp):
    return max(8, ((CAP_NUM * top_count * tok_count) // (CAP_DEN * n_exp) + 7) // 8 * 8)


def routing(idx_loc, gate_loc, n_exp, capacity):
    tok_count = idx_loc.shape[0]
    hit = idx_loc[:, :, None] == jnp.arange(n_exp, dtype=jnp.int32)[None, None, :]
    chosen = jnp.any(hit, axis=1)
    gates = jnp.sum(jnp.where(hit, gate_loc[:, :, None], 0.0), axis=1)
    before = jnp.tril(jnp.ones((tok_count, tok_count), jnp.bfloat16), -1)
    slot = jnp.dot(before, chosen.astype(jnp.bfloat16), preferred_element_type=jnp.float32).astype(jnp.int32)
    slot = jnp.where(chosen & (slot < capacity), slot, capacity)
    return slot.T, gates.T


def moe_kernel(x_in, slot_in, gate_in, ws_in, wg, wu, wd, acc, xr, ret, ws, w_v, pool, x_v, t_v, s_v, pre, h_v,
               w1s, w1r, w2s, w2r, w3s, w3r, lws, ds, dr, rs, rls, rr, xs, own, ss, sr, sl, sx):
    n_own = SIDE
    blk = wg.shape[2]
    n_src, cap, d_model = xr.shape[1:]
    tok_count = x_in.shape[0]
    unit = x_v.shape[1]
    units = n_src // unit
    d = lax.axis_index("data")
    p = lax.axis_index("expert")
    z, y = lax.div(d, SIDE), lax.rem(d, SIDE)
    x, c = lax.div(p, 2), lax.rem(p, 2)
    u = z * (1 - c) + y * c
    v = y * (1 - c) + z * c
    v_up, v_dn = lax.rem(v + 1, SIDE), lax.rem(v + SIDE - 1, SIDE)
    slots = lax.broadcasted_iota(jnp.int32, (cap, tok_count), 0)

    def data_of(uu, vv):
        return uu * (SIDE - 3 * c) + vv * (1 + 3 * c)

    def target(k):
        dx, cb, r = lax.rem(lax.div(k, 8) + 1, SIDE), lax.rem(lax.div(k, SIDE), 2), lax.rem(k, SIDE)
        tx, tc = lax.rem(x + dx, SIDE), lax.rem(c + cb, 2)
        tz = lax.rem(z + r * (1 - tc), SIDE)
        ty = lax.rem(y + r * tc, SIDE)
        tp = tx * 2 + tc
        return tp, tz * SIDE + ty, tp * (SIDE * n_own) + n_own * (tz * (1 - tc) + ty * tc)

    def source(k):
        dx, cb, r = lax.rem(lax.div(k, 8) + 1, SIDE), lax.rem(lax.div(k, SIDE), 2), lax.rem(k, SIDE)
        sp = lax.rem(x + SIDE - dx, SIDE) * 2 + lax.rem(c + cb, 2)
        return sp, data_of(lax.rem(u + SIDE - r, SIDE), v)

    def send(src, dst, s_sem, r_sem, data, expert):
        pltpu.make_async_remote_copy(src, dst, s_sem, r_sem, device_id={"data": data, "expert": expert}, device_id_type=MESH).start()

    def wait(ref, sem):
        pltpu.make_async_copy(ref, ref, sem).wait()

    def strips(e, count):
        return w_v.at[e, :, :, pl.ds(0, count * blk)]

    def strip(e, b):
        return w_v.at[e, :, :, pl.ds(pl.multiple_of(b * blk, blk), blk)]

    def part(e, i, b):
        return w_v.at[e, i, :, pl.ds(pl.multiple_of(b * blk, blk), blk)]

    def shared_own():
        return pltpu.make_async_copy(ws_in, ws.at[x, c, z, y], sl)

    def shared_sent(s, sem):
        wait((ws.at[0, 0, 0, pl.ds(0, 3)], ws.at[0, 0, pl.ds(0, 3)], ws.at[pl.ds(0, 3), 0], ws.at[:, 0])[s], sem.at[s])

    def shared_stage(s):
        if s == 0:
            shared_own().start()
            shared_own().wait()
        else:
            shared_sent(s - 1, sr)
        if s == 3:
            for core in range(2):
                @pl.when(c == core)
                def _(core=core):
                    send(ws.at[:, core], ws.at[:, core], ss.at[s], sr.at[s], d, p + 1 - 2 * core)
            return
        ref = (ws.at[x, c, z, y], ws.at[x, c, z], ws.at[x, c])[s]
        for r in range(1, SIDE):
            ty = lax.rem(y + r, SIDE) if s == 0 else y
            tz = lax.rem(z + r, SIDE) if s == 1 else z
            tx = lax.rem(x + r, SIDE) if s == 2 else x
            send(ref, ref, ss.at[s], sr.at[s], tz * SIDE + ty, tx * 2 + c)

    def shared_expert():
        shared_sent(3, sr)
        wide = h_v.shape[1]
        rows = s_v.shape[1] * s_v.shape[2] * s_v.shape[3]
        planes = d_model // rows
        nt = (((1,), (1,)), ((), ()))

        def fetch(g, s):
            return pltpu.make_async_copy(ws.at[lax.div(g, 2), lax.rem(g, 2)], s_v.at[s], sx.at[s])

        def over_planes(work):
            fetch(0, 0).start()

            def body(g, carry):
                s = lax.rem(g, 2)

                @pl.when(g + 1 < planes)
                def _():
                    fetch(g + 1, 1 - s).start()

                fetch(g, s).wait()
                work(g, pl.ds(pl.multiple_of(g * rows, rows), rows), s_v[s].reshape(rows, 3 * wide))
                return carry

            lax.fori_loop(0, planes, body, 0)

        pre[...] = jnp.zeros_like(pre)

        def gate_up(g, cols, blkw):
            pre[...] += jnp.dot(x_in[:, cols], blkw[:, :2 * wide], preferred_element_type=jnp.float32)

        def down(g, cols, blkw):
            acc[:, cols] += lax.dot_general(h_v[...], blkw[:, 2 * wide:], nt, preferred_element_type=jnp.float32)

        over_planes(gate_up)
        h_v[...] = (jax.nn.silu(pre[:, :wide]) * pre[:, wide:]).astype(jnp.bfloat16)
        over_planes(down)

    def start_trade(e):
        for i, w in enumerate((wg, wu, wd)):
            pltpu.make_async_copy(w.at[n_own * u + e], part(e, i, d), lws.at[e, i]).start()
        for r in range(1, SIDE):
            ut = lax.rem(u + r, SIDE)
            for i, w in enumerate((wg, wu, wd)):
                send(w.at[n_own * ut + e], part(e, i, d), w1s.at[e], w1r.at[e], data_of(ut, v), p)

    def start_rows(e, slot):
        def pick(g, carry):
            for j in range(unit):
                te = target(g * unit + j)[2] + e
                t_v[0, j * cap:(j + 1) * cap, :] = (slots == slot_in[pl.ds(te, 1), :]).astype(jnp.bfloat16)
            rows = jnp.dot(t_v[0], x_in[...], preferred_element_type=jnp.float32).astype(jnp.bfloat16)
            pool[slot, pl.ds(g * unit, unit)] = rows.reshape(unit, cap, d_model)
            return carry

        lax.fori_loop(0, units, pick, 0)

        def body(i, carry):
            k = i + lax.div(i, OWN)
            tp, td, _ = target(k)
            send(pool.at[slot, k], xr.at[e, k], ds.at[e], dr.at[e], td, tp)
            return carry

        lax.fori_loop(0, n_src - 1, body, 0)
        pltpu.make_async_copy(pool.at[slot, OWN], xr.at[e, OWN], own.at[e]).start()

    def wait_rows_sent(e, slot):
        wait(pool.at[slot, pl.ds(0, n_src - 1)], ds.at[e])
        pltpu.make_async_copy(pool.at[slot, OWN], xr.at[e, OWN], own.at[e]).wait()

    def start_gather(e):
        for i, w in enumerate((wg, wu, wd)):
            pltpu.make_async_copy(w.at[0], part(e, i, d), lws.at[e, i]).wait()
        wait(strips(e, 3), w1r.at[e])
        for i in range(SIDE):
            b = data_of(i, v)
            for vt in (v_up, v_dn):
                send(strip(e, b), strip(e, b), w2s.at[e], w2r.at[e], data_of(u, vt), p)

    def start_relay(e):
        wait(strips(e, 8), w2r.at[e])
        for i in range(SIDE):
            vs, vt = (v_dn, v_up) if i < SIDE // 2 else (v_up, v_dn)
            b = data_of(i, vs)
            send(strip(e, b), strip(e, b), w3s.at[e], w3r.at[e], data_of(u, vt), p)

    def load(src, e, g, s):
        return pltpu.make_async_copy(src.at[e, pl.ds(g * unit, unit)], x_v.at[s], xs.at[s])

    def arrived(src, e, work, landed):
        def body(i, carry):
            s, g = lax.rem(i, 2), lax.rem(i + 3, units)
            landed(g)
            load(src, e, g, s).start()
            load(src, e, g, s).wait()
            work(g, x_v[s].reshape(unit * cap, d_model))
            return carry

        lax.fori_loop(0, units, body, 0)

    def streamed(src, e, work):
        load(src, e, 0, 0).start()

        def body(g, carry):
            s = lax.rem(g, 2)

            @pl.when(g + 1 < units)
            def _():
                load(src, e, g + 1, 1 - s).start()

            load(src, e, g, s).wait()
            work(g, x_v[s].reshape(unit * cap, d_model))
            return carry

        lax.fori_loop(0, units, body, 0)

    def give_back(e, slot, k):
        sp, sd = source(k)
        send(pool.at[slot, k], ret.at[e, k], rs.at[e], rr.at[e, k // unit], sd, sp)

    def experts(e, slot):
        wait(strips(e, 4), w3r.at[e])
        wait(xr.at[e, pl.ds(0, n_src - 1)], dr.at[e])
        nt = (((1,), (1,)), ((), ()))

        def send_unit(g, skip=0):
            for j in range(skip, unit):
                give_back(e, slot, g * unit + j)

        def work(g, rows):
            gate_pre = lax.dot_general(rows, w_v[e, 0], nt, preferred_element_type=jnp.float32)
            up_pre = lax.dot_general(rows, w_v[e, 1], nt, preferred_element_type=jnp.float32)
            hidden = (jax.nn.silu(gate_pre) * up_pre).astype(jnp.bfloat16)
            res = jnp.dot(hidden, w_v[e, 2], preferred_element_type=jnp.float32).astype(jnp.bfloat16)
            pool[slot, pl.ds(g * unit, unit)] = res.reshape(unit, cap, d_model)

            @pl.when(g > 0)
            def _():
                send_unit(g - 1)

        streamed(xr, e, work)
        send_unit(units - 1, 1)
        pltpu.make_async_copy(pool.at[slot, OWN], ret.at[e, OWN], rls.at[e]).start()

    def wait_results_sent(e, slot):
        wait(pool.at[slot, pl.ds(0, n_src - 1)], rs.at[e])

    def combine(e):
        pltpu.make_async_copy(pool.at[0, OWN], ret.at[e, OWN], rls.at[e]).wait()

        def landed(g):
            for last in range(2):
                @pl.when((g == units - 1) if last else (g < units - 1))
                def _(last=last):
                    wait(ret.at[e, pl.ds(0, unit - last)], rr.at[e, g])

        tn = (((0,), (0,)), ((), ()))
        width = d_model // 4

        def work(g, rows):
            for j in range(unit):
                te = target(g * unit + j)[2] + e
                val = jnp.where(slots == slot_in[pl.ds(te, 1), :], gate_in[pl.ds(te, 1), :], 0.0)
                hi = val.astype(jnp.bfloat16)
                rest = val - hi.astype(jnp.float32)
                mid = rest.astype(jnp.bfloat16)
                low = (rest - mid.astype(jnp.float32)).astype(jnp.bfloat16)
                for i, term in enumerate((hi, mid, low)):
                    t_v[i, j * cap:(j + 1) * cap, :] = term
            for n in range(4):
                cols = rows[:, n * width:(n + 1) * width]
                total = acc[:, n * width:(n + 1) * width]
                for i in range(3):
                    total += lax.dot_general(t_v[i], cols, tn, preferred_element_type=jnp.float32)
                acc[:, n * width:(n + 1) * width] = total

        if isinstance(e, int):
            arrived(ret, e, work, landed)
        else:
            for g in range(units):
                landed(g)
            streamed(ret, e, work)

    start_trade(0)
    start_rows(0, 0)
    shared_stage(0)
    start_trade(1)
    start_rows(1, 1)
    acc[...] = x_in[...].astype(jnp.float32)
    start_gather(0)
    start_trade(2)
    start_rows(2, 2)
    start_relay(0)
    shared_stage(1)
    start_gather(1)
    start_trade(3)
    wait_rows_sent(0, 0)
    start_rows(3, 0)

    def step(e, carry):
        slot = lax.rem(e + 1, 3)

        @pl.when(e < 3)
        def _():
            wait_rows_sent(e + 1, slot)

        @pl.when(e == 3)
        def _():
            wait_results_sent(0, 1)

        experts(e, slot)

        @pl.when(e + 1 < n_own)
        def _():
            start_relay(e + 1)

        @pl.when(e + 2 < n_own)
        def _():
            start_gather(e + 2)

        @pl.when(e == 0)
        def _():
            shared_stage(2)

        @pl.when(e == 1)
        def _():
            combine(e - 1)

        return carry

    lax.fori_loop(0, n_own, step, 0)
    shared_stage(3)
    lax.fori_loop(1, 2, lambda e, carry: combine(e) or carry, 0)
    shared_expert()
    lax.fori_loop(2, 3, lambda e, carry: combine(e) or carry, 0)
    combine(n_own - 1)
    for e in range(1, n_own):
        wait_results_sent(e, (e + 1) % 3)

    def drain(e, carry):
        wait(strips(e, 3), w1s.at[e])
        wait(strips(e, 8), w2s.at[e])
        wait(strips(e, 4), w3s.at[e])
        return carry

    lax.fori_loop(0, n_own, drain, 0)
    for s in range(4):
        shared_sent(s, ss)


def moe(x_loc, slot, gates, ws_loc, wg_loc, wu_loc, wd_loc, cap):
    tok_count, d_model = x_loc.shape
    n_loc, blk, ff = wg_loc.shape
    n_exp = slot.shape[0]
    n_own, n_src, unit = SIDE, 8 * SIDE, 8
    dma = pltpu.SemaphoreType.DMA
    bf16 = jnp.bfloat16
    any_spec = pl.BlockSpec(memory_space=pl.ANY)
    vmem_spec = pl.BlockSpec(memory_space=pltpu.VMEM)
    stage = jax.ShapeDtypeStruct((n_own, n_src, cap, d_model), bf16)
    return pl.pallas_call(
        moe_kernel,
        out_shape=(jax.ShapeDtypeStruct((tok_count, d_model), jnp.float32), stage, stage, jax.ShapeDtypeStruct((SIDE, 2, SIDE, SIDE) + ws_loc.shape, bf16)),
        in_specs=[vmem_spec] * 4 + [any_spec] * 3,
        out_specs=(vmem_spec, any_spec, any_spec, any_spec),
        scratch_shapes=[
            pltpu.VMEM((n_own, 3, ff, d_model), bf16),
            pltpu.VMEM((3, n_src, cap, d_model), bf16),
            pltpu.VMEM((2, unit, cap, d_model), bf16),
            pltpu.VMEM((3, unit * cap, tok_count), bf16),
            pltpu.VMEM((2, SIDE, SIDE) + ws_loc.shape, bf16),
            pltpu.VMEM((tok_count, ws_loc.shape[1] // 3 * 2), jnp.float32),
            pltpu.VMEM((tok_count, ws_loc.shape[1] // 3), bf16),
        ] + [dma((n_own,))] * 6 + [dma((n_own, 3))] + [dma((n_own,))] * 4 + [dma((n_own, n_src // unit)), dma((2,)), dma((n_own,)), dma((4,)), dma((4,)), dma, dma((2,))],
        compiler_params=pltpu.CompilerParams(has_side_effects=True, vmem_limit_bytes=65400 * 1024),
        cost_estimate=pl.CostEstimate(flops=60 * n_exp * cap * d_model * ff, bytes_accessed=100_000_000, transcendentals=n_exp * cap * ff),
        name="moe_exchange",
    )(x_loc, slot, gates, ws_loc, jnp.swapaxes(wg_loc, 1, 2), jnp.swapaxes(wu_loc, 1, 2), wd_loc)[0]


def solution(mesh):
    exp_n = mesh.shape["expert"]
    tok_spec = P(("rep", "expert", "data"), None)
    group_axes = ("expert", "data")

    def device_fn(x_loc, idx_loc, gate_loc, wg_loc, wu_loc, wd_loc, wsg_loc, wsu_loc, wsd_loc):
        tok_count, d_model = x_loc.shape
        n_exp = wg_loc.shape[0] * exp_n
        ff_shared = wsg_loc.shape[1]
        capacity = capacity_of(tok_count, idx_loc.shape[1], n_exp)
        pad = -ff_shared % 128
        ws_loc = jnp.concatenate([jnp.pad(w, ((0, 0), (0, pad))) for w in (wsg_loc, wsu_loc, wsd_loc.T)], axis=1)
        slot, gates = routing(idx_loc, gate_loc, n_exp, capacity)
        return moe(x_loc, slot, gates, ws_loc, wg_loc, wu_loc, wd_loc, capacity).astype(jnp.bfloat16)

    in_specs = (tok_spec, tok_spec, tok_spec, P("expert", "data", None), P("expert", "data", None), P("expert", None, "data"), P(group_axes, None), P(group_axes, None), P(None, group_axes))
    return jax.shard_map(device_fn, mesh=mesh, in_specs=in_specs, out_specs=tok_spec, check_vma=False)
```

```python
import jax
import jax.numpy as jnp
from jax import lax
from jax.experimental import pallas as pl
from jax.experimental.pallas import tpu as pltpu
from jax.sharding import PartitionSpec as P

MESH = pl.DeviceIdType.MESH
OWN = 24
CAP_NUM = 5
CAP_DEN = 4
SIDE = 4


def capacity_of(tok_count, top_count, n_exp):
    return max(8, ((CAP_NUM * top_count * tok_count) // (CAP_DEN * n_exp) + 7) // 8 * 8)


def routing(idx_loc, gate_loc, n_exp, capacity):
    tok_count = idx_loc.shape[0]
    hit = idx_loc[:, :, None] == jnp.arange(n_exp, dtype=jnp.int32)[None, None, :]
    chosen = jnp.any(hit, axis=1)
    gates = jnp.sum(jnp.where(hit, gate_loc[:, :, None], 0.0), axis=1)
    before = jnp.tril(jnp.ones((tok_count, tok_count), jnp.bfloat16), -1)
    slot = jnp.dot(before, chosen.astype(jnp.bfloat16), preferred_element_type=jnp.float32).astype(jnp.int32)
    slot = jnp.where(chosen & (slot < capacity), slot, capacity)
    return slot.T, gates.T


def moe_kernel(x_in, slot_in, gate_in, ws_in, wg, wu, wd, acc, xr, ret, ws, w_v, pool, x_v, t_v, s_v, pre, h_v,
               w1s, w1r, w2s, w2r, w3s, w3r, lws, ds, dr, rs, rls, rr, xs, own, ss, sr, sl, sx):
    n_own = SIDE
    blk = wg.shape[2]
    n_src, cap, d_model = xr.shape[1:]
    tok_count = x_in.shape[0]
    unit = x_v.shape[1]
    units = n_src // unit
    d = lax.axis_index("data")
    p = lax.axis_index("expert")
    z, y = lax.div(d, SIDE), lax.rem(d, SIDE)
    x, c = lax.div(p, 2), lax.rem(p, 2)
    u = z * (1 - c) + y * c
    v = y * (1 - c) + z * c
    v_up, v_dn = lax.rem(v + 1, SIDE), lax.rem(v + SIDE - 1, SIDE)
    slots = lax.broadcasted_iota(jnp.int32, (cap, tok_count), 0)

    def data_of(uu, vv):
        return uu * (SIDE - 3 * c) + vv * (1 + 3 * c)

    def target(k):
        dx, cb, r = lax.rem(lax.div(k, 8) + 1, SIDE), lax.rem(lax.div(k, SIDE), 2), lax.rem(k, SIDE)
        tx, tc = lax.rem(x + dx, SIDE), lax.rem(c + cb, 2)
        tz = lax.rem(z + r * (1 - tc), SIDE)
        ty = lax.rem(y + r * tc, SIDE)
        tp = tx * 2 + tc
        return tp, tz * SIDE + ty, tp * (SIDE * n_own) + n_own * (tz * (1 - tc) + ty * tc)

    def source(k):
        dx, cb, r = lax.rem(lax.div(k, 8) + 1, SIDE), lax.rem(lax.div(k, SIDE), 2), lax.rem(k, SIDE)
        sp = lax.rem(x + SIDE - dx, SIDE) * 2 + lax.rem(c + cb, 2)
        return sp, data_of(lax.rem(u + SIDE - r, SIDE), v)

    def send(src, dst, s_sem, r_sem, data, expert):
        pltpu.make_async_remote_copy(src, dst, s_sem, r_sem, device_id={"data": data, "expert": expert}, device_id_type=MESH).start()

    def wait(ref, sem):
        pltpu.make_async_copy(ref, ref, sem).wait()

    def strips(e, count):
        return w_v.at[e, :, :, pl.ds(0, count * blk)]

    def strip(e, b):
        return w_v.at[e, :, :, pl.ds(pl.multiple_of(b * blk, blk), blk)]

    def part(e, i, b):
        return w_v.at[e, i, :, pl.ds(pl.multiple_of(b * blk, blk), blk)]

    def shared_own():
        return pltpu.make_async_copy(ws_in, ws.at[x, c, z, y], sl)

    def shared_sent(s, sem):
        wait((ws.at[0, 0, 0, pl.ds(0, 3)], ws.at[0, 0, pl.ds(0, 3)], ws.at[pl.ds(0, 3), 0], ws.at[:, 0])[s], sem.at[s])

    def shared_stage(s):
        if s == 0:
            shared_own().start()
            shared_own().wait()
        else:
            shared_sent(s - 1, sr)
        if s == 3:
            for core in range(2):
                @pl.when(c == core)
                def _(core=core):
                    send(ws.at[:, core], ws.at[:, core], ss.at[s], sr.at[s], d, p + 1 - 2 * core)
            return
        ref = (ws.at[x, c, z, y], ws.at[x, c, z], ws.at[x, c])[s]
        for r in range(1, SIDE):
            ty = lax.rem(y + r, SIDE) if s == 0 else y
            tz = lax.rem(z + r, SIDE) if s == 1 else z
            tx = lax.rem(x + r, SIDE) if s == 2 else x
            send(ref, ref, ss.at[s], sr.at[s], tz * SIDE + ty, tx * 2 + c)

    def shared_expert():
        shared_sent(3, sr)
        wide = h_v.shape[1]
        rows = s_v.shape[1] * s_v.shape[2] * s_v.shape[3]
        planes = d_model // rows
        nt = (((1,), (1,)), ((), ()))

        def fetch(g, s):
            return pltpu.make_async_copy(ws.at[lax.div(g, 2), lax.rem(g, 2)], s_v.at[s], sx.at[s])

        def over_planes(work):
            fetch(0, 0).start()

            def body(g, carry):
                s = lax.rem(g, 2)

                @pl.when(g + 1 < planes)
                def _():
                    fetch(g + 1, 1 - s).start()

                fetch(g, s).wait()
                work(g, pl.ds(pl.multiple_of(g * rows, rows), rows), s_v[s].reshape(rows, 3 * wide))
                return carry

            lax.fori_loop(0, planes, body, 0)

        pre[...] = jnp.zeros_like(pre)

        def gate_up(g, cols, blkw):
            pre[...] += jnp.dot(x_in[:, cols], blkw[:, :2 * wide], preferred_element_type=jnp.float32)

        def down(g, cols, blkw):
            acc[:, cols] += lax.dot_general(h_v[...], blkw[:, 2 * wide:], nt, preferred_element_type=jnp.float32)

        over_planes(gate_up)
        h_v[...] = (jax.nn.silu(pre[:, :wide]) * pre[:, wide:]).astype(jnp.bfloat16)
        over_planes(down)

    def start_trade(e):
        for i, w in enumerate((wg, wu, wd)):
            pltpu.make_async_copy(w.at[n_own * u + e], part(e, i, d), lws.at[e, i]).start()
        for r in range(1, SIDE):
            ut = lax.rem(u + r, SIDE)
            for i, w in enumerate((wg, wu, wd)):
                send(w.at[n_own * ut + e], part(e, i, d), w1s.at[e], w1r.at[e], data_of(ut, v), p)

    def start_rows(e, slot):
        def pick(g, carry):
            for j in range(unit):
                te = target(g * unit + j)[2] + e
                t_v[0, j * cap:(j + 1) * cap, :] = (slots == slot_in[pl.ds(te, 1), :]).astype(jnp.bfloat16)
            rows = jnp.dot(t_v[0], x_in[...], preferred_element_type=jnp.float32).astype(jnp.bfloat16)
            pool[slot, pl.ds(g * unit, unit)] = rows.reshape(unit, cap, d_model)
            return carry

        lax.fori_loop(0, units, pick, 0)

        def body(i, carry):
            k = i + lax.div(i, OWN)
            tp, td, _ = target(k)
            send(pool.at[slot, k], xr.at[e, k], ds.at[e], dr.at[e], td, tp)
            return carry

        lax.fori_loop(0, n_src - 1, body, 0)
        pltpu.make_async_copy(pool.at[slot, OWN], xr.at[e, OWN], own.at[e]).start()

    def wait_rows_sent(e, slot):
        wait(pool.at[slot, pl.ds(0, n_src - 1)], ds.at[e])
        pltpu.make_async_copy(pool.at[slot, OWN], xr.at[e, OWN], own.at[e]).wait()

    def start_gather(e):
        for i, w in enumerate((wg, wu, wd)):
            pltpu.make_async_copy(w.at[0], part(e, i, d), lws.at[e, i]).wait()
        wait(strips(e, 3), w1r.at[e])
        for i in range(SIDE):
            b = data_of(i, v)
            for vt in (v_up, v_dn):
                send(strip(e, b), strip(e, b), w2s.at[e], w2r.at[e], data_of(u, vt), p)

    def start_relay(e):
        wait(strips(e, 8), w2r.at[e])
        for i in range(SIDE):
            vs, vt = (v_dn, v_up) if i < SIDE // 2 else (v_up, v_dn)
            b = data_of(i, vs)
            send(strip(e, b), strip(e, b), w3s.at[e], w3r.at[e], data_of(u, vt), p)

    def load(src, e, g, s):
        return pltpu.make_async_copy(src.at[e, pl.ds(g * unit, unit)], x_v.at[s], xs.at[s])

    def arrived(src, e, work, landed):
        def body(i, carry):
            s, g = lax.rem(i, 2), lax.rem(i + 3, units)
            landed(g)
            load(src, e, g, s).start()
            load(src, e, g, s).wait()
            work(g, x_v[s].reshape(unit * cap, d_model))
            return carry

        lax.fori_loop(0, units, body, 0)

    def streamed(src, e, work):
        load(src, e, 0, 0).start()

        def body(g, carry):
            s = lax.rem(g, 2)

            @pl.when(g + 1 < units)
            def _():
                load(src, e, g + 1, 1 - s).start()

            load(src, e, g, s).wait()
            work(g, x_v[s].reshape(unit * cap, d_model))
            return carry

        lax.fori_loop(0, units, body, 0)

    def give_back(e, slot, k):
        sp, sd = source(k)
        send(pool.at[slot, k], ret.at[e, k], rs.at[e], rr.at[e, k // unit], sd, sp)

    def experts(e, slot):
        wait(strips(e, 4), w3r.at[e])
        wait(xr.at[e, pl.ds(0, n_src - 1)], dr.at[e])
        nt = (((1,), (1,)), ((), ()))

        def send_unit(g, skip=0):
            for j in range(skip, unit):
                give_back(e, slot, g * unit + j)

        def work(g, rows):
            gate_pre = lax.dot_general(rows, w_v[e, 0], nt, preferred_element_type=jnp.float32)
            up_pre = lax.dot_general(rows, w_v[e, 1], nt, preferred_element_type=jnp.float32)
            hidden = (jax.nn.silu(gate_pre) * up_pre).astype(jnp.bfloat16)
            res = jnp.dot(hidden, w_v[e, 2], preferred_element_type=jnp.float32).astype(jnp.bfloat16)
            pool[slot, pl.ds(g * unit, unit)] = res.reshape(unit, cap, d_model)

            @pl.when(g > 0)
            def _():
                send_unit(g - 1)

        streamed(xr, e, work)
        send_unit(units - 1, 1)
        pltpu.make_async_copy(pool.at[slot, OWN], ret.at[e, OWN], rls.at[e]).start()

    def wait_results_sent(e, slot):
        wait(pool.at[slot, pl.ds(0, n_src - 1)], rs.at[e])

    def combine(e):
        pltpu.make_async_copy(pool.at[0, OWN], ret.at[e, OWN], rls.at[e]).wait()

        def landed(g):
            for last in range(2):
                @pl.when((g == units - 1) if last else (g < units - 1))
                def _(last=last):
                    wait(ret.at[e, pl.ds(0, unit - last)], rr.at[e, g])

        tn = (((0,), (0,)), ((), ()))
        width = d_model // 4

        def work(g, rows):
            for j in range(unit):
                te = target(g * unit + j)[2] + e
                val = jnp.where(slots == slot_in[pl.ds(te, 1), :], gate_in[pl.ds(te, 1), :], 0.0)
                hi = val.astype(jnp.bfloat16)
                rest = val - hi.astype(jnp.float32)
                mid = rest.astype(jnp.bfloat16)
                low = (rest - mid.astype(jnp.float32)).astype(jnp.bfloat16)
                for i, term in enumerate((hi, mid, low)):
                    t_v[i, j * cap:(j + 1) * cap, :] = term
            for n in range(4):
                cols = rows[:, n * width:(n + 1) * width]
                total = acc[:, n * width:(n + 1) * width]
                for i in range(3):
                    total += lax.dot_general(t_v[i], cols, tn, preferred_element_type=jnp.float32)
                acc[:, n * width:(n + 1) * width] = total

        if isinstance(e, int):
            arrived(ret, e, work, landed)
        else:
            for g in range(units):
                landed(g)
            streamed(ret, e, work)

    start_trade(0)
    start_rows(0, 0)
    shared_stage(0)
    start_trade(1)
    start_rows(1, 1)
    acc[...] = x_in[...].astype(jnp.float32)
    start_gather(0)
    start_trade(2)
    start_rows(2, 2)
    start_relay(0)
    shared_stage(1)
    start_gather(1)
    start_trade(3)
    wait_rows_sent(0, 0)
    start_rows(3, 0)

    def step(e, carry):
        slot = lax.rem(e + 1, 3)

        @pl.when(e < 3)
        def _():
            wait_rows_sent(e + 1, slot)

        @pl.when(e == 3)
        def _():
            wait_results_sent(0, 1)

        experts(e, slot)

        @pl.when(e + 1 < n_own)
        def _():
            start_relay(e + 1)

        @pl.when(e + 2 < n_own)
        def _():
            start_gather(e + 2)

        @pl.when(e == 0)
        def _():
            shared_stage(2)

        @pl.when(e == 3)
        def _():
            shared_expert()

        @pl.when(e >= 1)
        def _():
            combine(e - 1)

        @pl.when(e == 2)
        def _():
            shared_stage(3)

        return carry

    lax.fori_loop(0, n_own, step, 0)
    combine(n_own - 1)
    for e in range(1, n_own):
        wait_results_sent(e, (e + 1) % 3)

    def drain(e, carry):
        wait(strips(e, 3), w1s.at[e])
        wait(strips(e, 8), w2s.at[e])
        wait(strips(e, 4), w3s.at[e])
        return carry

    lax.fori_loop(0, n_own, drain, 0)
    for s in range(4):
        shared_sent(s, ss)


def moe(x_loc, slot, gates, ws_loc, wg_loc, wu_loc, wd_loc, cap):
    tok_count, d_model = x_loc.shape
    n_loc, blk, ff = wg_loc.shape
    n_exp = slot.shape[0]
    n_own, n_src, unit = SIDE, 8 * SIDE, 8
    dma = pltpu.SemaphoreType.DMA
    bf16 = jnp.bfloat16
    any_spec = pl.BlockSpec(memory_space=pl.ANY)
    vmem_spec = pl.BlockSpec(memory_space=pltpu.VMEM)
    stage = jax.ShapeDtypeStruct((n_own, n_src, cap, d_model), bf16)
    return pl.pallas_call(
        moe_kernel,
        out_shape=(jax.ShapeDtypeStruct((tok_count, d_model), jnp.float32), stage, stage, jax.ShapeDtypeStruct((SIDE, 2, SIDE, SIDE) + ws_loc.shape, bf16)),
        in_specs=[vmem_spec] * 4 + [any_spec] * 3,
        out_specs=(vmem_spec, any_spec, any_spec, any_spec),
        scratch_shapes=[
            pltpu.VMEM((n_own, 3, ff, d_model), bf16),
            pltpu.VMEM((3, n_src, cap, d_model), bf16),
            pltpu.VMEM((2, unit, cap, d_model), bf16),
            pltpu.VMEM((3, unit * cap, tok_count), bf16),
            pltpu.VMEM((2, SIDE, SIDE) + ws_loc.shape, bf16),
            pltpu.VMEM((tok_count, ws_loc.shape[1] // 3 * 2), jnp.float32),
            pltpu.VMEM((tok_count, ws_loc.shape[1] // 3), bf16),
        ] + [dma((n_own,))] * 6 + [dma((n_own, 3))] + [dma((n_own,))] * 4 + [dma((n_own, n_src // unit)), dma((2,)), dma((n_own,)), dma((4,)), dma((4,)), dma, dma((2,))],
        compiler_params=pltpu.CompilerParams(has_side_effects=True, vmem_limit_bytes=65400 * 1024),
        cost_estimate=pl.CostEstimate(flops=60 * n_exp * cap * d_model * ff, bytes_accessed=100_000_000, transcendentals=n_exp * cap * ff),
        name="moe_exchange",
    )(x_loc, slot, gates, ws_loc, jnp.swapaxes(wg_loc, 1, 2), jnp.swapaxes(wu_loc, 1, 2), wd_loc)[0]


def solution(mesh):
    exp_n = mesh.shape["expert"]
    tok_spec = P(("rep", "expert", "data"), None)
    group_axes = ("expert", "data")

    def device_fn(x_loc, idx_loc, gate_loc, wg_loc, wu_loc, wd_loc, wsg_loc, wsu_loc, wsd_loc):
        tok_count, d_model = x_loc.shape
        n_exp = wg_loc.shape[0] * exp_n
        ff_shared = wsg_loc.shape[1]
        capacity = capacity_of(tok_count, idx_loc.shape[1], n_exp)
        pad = -ff_shared % 128
        ws_loc = jnp.concatenate([jnp.pad(w, ((0, 0), (0, pad))) for w in (wsg_loc, wsu_loc, wsd_loc.T)], axis=1)
        slot, gates = routing(idx_loc, gate_loc, n_exp, capacity)
        return moe(x_loc, slot, gates, ws_loc, wg_loc, wu_loc, wd_loc, capacity).astype(jnp.bfloat16)

    in_specs = (tok_spec, tok_spec, tok_spec, P("expert", "data", None), P("expert", "data", None), P("expert", None, "data"), P(group_axes, None), P(group_axes, None), P(None, group_axes))
    return jax.shard_map(device_fn, mesh=mesh, in_specs=in_specs, out_specs=tok_spec, check_vma=False)
```
